32 devices in a mesh: graphs: 2 (over y), rows: 4 (over z), cols: 2 (over x), sub: 2 (over core).
Axes of the slice: x: 2, y: 2, z: 4, core: 2. Of those that a mesh axis runs over, the one named last changes fastest.
Arguments:
- current_block: float32 [16, 65536], P(None, ('graphs', 'rows', 'cols', 'sub')), parts along dimension 1, may hold values from -1200 to 1200, as said below
- previous_block: float32 [16, 65536], P(None, ('graphs', 'rows', 'cols', 'sub')), parts along dimension 1, may hold values from -1200 to 1200, as said below
- adjacency_tiles: float32 [1536, 128, 128], P(('graphs', 'rows', 'cols', 'sub')), parts along dimension 0, may hold values from -0.3125 to 0.3125
- tile_rows: int32 [1536], P(('graphs', 'rows', 'cols', 'sub')), parts along dimension 0, may hold values from 0 to 255, as said below
- tile_cols: int32 [1536], P(('graphs', 'rows', 'cols', 'sub')), parts along dimension 0, may hold values from 0 to 255, as said below
- tile_count: int32 [32], P(('graphs', 'rows', 'cols', 'sub')), parts along dimension 0, may hold values from 18 to 48, as said below
- locked: int32 [2], P('graphs'), parts along dimension 0, may hold values from 0 to 7
Outputs:
- w_basis: float32 [16, 65536], P(None, ('graphs', 'rows', 'cols', 'sub')), parts along dimension 1
- w_image: float32 [16, 65536], P(None, ('graphs', 'rows', 'cols', 'sub')), parts along dimension 1
- ritz_matrix: float32 [96, 48], P('graphs'), parts along dimension 0
The draws below stay inside these ranges and needn't reach their ends.
There are 2 independent parts, one for each index of `graphs`. The reference program is written for one: setup_inputs(seed, part) draws one part's arguments, and reference() takes and returns one part's arrays. A program takes and returns all parts, laid end to end along the dimension named above; each array names one. Nothing has to cross between parts.
Inputs may be any that keep to these rules, and one draw needn't show every extreme that they name: `current_block`: entries of order one to some hundreds. `previous_block`: entries of order one to some hundreds. Slots d * 48 to (d + 1) * 48 - 1 belong to device d and name its own tile rows d * 16 to (d + 1) * 16 - 1. The first 16 slots of a device name its tile rows in order, with tile_cols equal to tile_rows. Slots past the device's count name tile row d * 16 and carry no weight. `tile_cols`: A slot of device d names a tile column from d * 16 - 8 to (d + 1) * 16 + 7. Slot 16 of a device names a tile of the block before it and slot 17 one of the block after it, where such a block exists. A pair of tile row and tile column may stand in several slots; their tiles add. `tile_count`: in every draw some device has all 48 slots live.
All inputs are finite; a program needn't handle non-finite values.
Results may differ from the reference program's by a relative error of at most 0.000094.
Values sent between devices are 32-bit elements; how exact they have to be, the bound alone decides.
A program may use at most 64 MiB of HBM per device.

```python
import jax
import jax.numpy as jnp
from jax import lax

K = 16
TILE_VERTICES = 128
DEVICE_SLOTS = 3
DEVS = 16
DEVICE_TILE_ROWS = 16
REACH = 8
MAXT_DEV = 48
NV = 32768
NT = 256
GRAPH_SLOTS = 768


def tile_arrangement(key):
    keys = jax.random.split(jax.random.fold_in(key, 11), 6)
    devices = jnp.arange(DEVS, dtype=jnp.int32)
    slot_indices = jnp.arange(MAXT_DEV, dtype=jnp.int32)[None, :]
    extra = jax.random.randint(keys[0], (DEVS,), 2, MAXT_DEV - DEVICE_TILE_ROWS + 1)
    fullest = jax.random.randint(keys[1], (), 0, DEVS)
    extra = jnp.where(devices == fullest, MAXT_DEV - DEVICE_TILE_ROWS, extra)
    counts = (DEVICE_TILE_ROWS + extra).astype(jnp.int32)
    row_offset = jax.random.randint(keys[2], (DEVS, MAXT_DEV), 0, DEVICE_TILE_ROWS)
    col_offset = jax.random.randint(keys[3], (DEVS, MAXT_DEV), -REACH, DEVICE_TILE_ROWS + REACH)
    left_offset = jax.random.randint(keys[4], (DEVS, MAXT_DEV), -REACH, 0)
    right_offset = DEVICE_TILE_ROWS + jax.random.randint(keys[5], (DEVS, MAXT_DEV), 0, REACH)
    col_offset = jnp.where(slot_indices == DEVICE_TILE_ROWS, left_offset, col_offset)
    col_offset = jnp.where(slot_indices == DEVICE_TILE_ROWS + 1, right_offset, col_offset)
    diagonal = slot_indices < DEVICE_TILE_ROWS
    row_offset = jnp.where(diagonal, slot_indices, row_offset)
    col_offset = jnp.where(diagonal, slot_indices, col_offset)
    padded = slot_indices >= counts[:, None]
    row_offset = jnp.where(padded, 0, row_offset)
    col_offset = jnp.where(padded, 0, col_offset)
    rows_out = devices[:, None] * DEVICE_TILE_ROWS + row_offset
    cols_out = devices[:, None] * DEVICE_TILE_ROWS + col_offset
    cols_out = jnp.where(cols_out < 0, cols_out + REACH, cols_out)
    cols_out = jnp.where(cols_out >= NT, cols_out - REACH, cols_out)
    return (rows_out.reshape(-1).astype(jnp.int32), cols_out.reshape(-1).astype(jnp.int32), counts)


def draw_tile_rows(key, part):
    return tile_arrangement(key)[0]


def draw_tile_cols(key, part):
    return tile_arrangement(key)[1]


def draw_tile_count(key, part):
    return tile_arrangement(key)[2]


def draw_locked(key, part):
    base = jax.random.randint(jax.random.fold_in(key, 53), (1,), 0, 7)
    return jnp.where(part % 2 == 1, 7, base).astype(jnp.int32)


def vector_draw(key):
    keys = jax.random.split(key, 4)
    where_along = jnp.arange(NV, dtype=jnp.float32) / NV
    rising = jnp.sqrt(1.0 + 2.0 * where_along)
    base = jax.random.truncated_normal(keys[0], -5.0, 5.0, (K, NV), jnp.float32)
    rough = 10.0 ** jax.random.uniform(keys[2], (NV,), jnp.float32)
    column_scale = 10.0 ** jax.random.uniform(keys[3], (K,), jnp.float32)
    return base * (rough * rising)[None, :] * column_scale[:, None]


def draw_current_block(key, part):
    return vector_draw(jax.random.fold_in(key, 21))


def draw_previous_block(key, part):
    return vector_draw(jax.random.fold_in(key, 37))


def shard_levels(rng, dims, cuts, smallest, high):
    loudness = 1.0
    for dim, blocks in cuts:
        draws = jax.random.uniform(jax.random.fold_in(jax.random.fold_in(rng, 6), dim), (blocks,), jnp.float32, smallest / len(cuts), high / len(cuts))
        loudness = loudness * jnp.repeat(jnp.exp(draws), dims[dim] // blocks).reshape((-1,) + (1,) * (len(dims) - 1 - dim))
    return loudness


def normal_values(rng, dims, spread, most, shards=(), kind=jnp.bfloat16):
    drawn = spread * jax.random.normal(rng, dims, jnp.float32)
    if shards:
        drawn = drawn * shard_levels(rng, dims, shards, -0.22, 0.18)
    return jnp.clip(drawn, -most, most).astype(kind)


def setup_inputs(seed: int = 0, part: int = 0) -> dict:
    splits = jax.random.split(jax.random.key(seed), 8)
    own_keys = jax.random.split(jax.random.fold_in(splits[7], part), 8)
    return {
        "current_block": draw_current_block(jax.random.fold_in(jax.random.fold_in(splits[7], part), 71), part),
        "previous_block": draw_previous_block(jax.random.fold_in(jax.random.fold_in(splits[7], part), 71), part),
        "adjacency_tiles": normal_values(own_keys[2], (GRAPH_SLOTS, TILE_VERTICES, TILE_VERTICES), (DEVICE_SLOTS * TILE_VERTICES) ** -0.5, 0.3125, ((0, 16),), jnp.float32),
        "tile_rows": draw_tile_rows(jax.random.fold_in(jax.random.fold_in(splits[7], part), 71), part),
        "tile_cols": draw_tile_cols(jax.random.fold_in(jax.random.fold_in(splits[7], part), 71), part),
        "tile_count": draw_tile_count(jax.random.fold_in(jax.random.fold_in(splits[7], part), 71), part),
        "locked": draw_locked(jax.random.fold_in(jax.random.fold_in(splits[7], part), 71), part),
    }


def apply_operator(vectors, adjacency_tiles, tile_rows, tile_cols, live_mask):
    channels = vectors.shape[0]
    column_blocks = vectors.reshape(channels, NT, TILE_VERTICES)
    gathered = jnp.take(column_blocks, tile_cols, axis=1)
    products = jnp.einsum('cta,tab->tcb', gathered, adjacency_tiles, precision=lax.Precision.HIGHEST)
    products = products * live_mask[:, None, None]
    summed = jax.ops.segment_sum(products, tile_rows, num_segments=NT)
    return vectors - jnp.transpose(summed, (1, 0, 2)).reshape(channels, NV)

def inner_products(left, right):
    return jnp.dot(left, right.T, precision=lax.Precision.HIGHEST)

def rayleigh_ritz(gram_b, gram_a):
    factor_b = jnp.linalg.cholesky(gram_b)
    symmetric = 0.5 * (gram_a + gram_a.T)
    halfway = lax.linalg.triangular_solve(factor_b, symmetric, left_side=True, lower=True)
    return lax.linalg.triangular_solve(factor_b, halfway.T, left_side=True, lower=True)

def reference(current_block, previous_block, adjacency_tiles, tile_rows, tile_cols, tile_count, locked):
    slot_indices = jnp.arange(GRAPH_SLOTS, dtype=jnp.int32)
    owners = slot_indices // MAXT_DEV
    live_mask = (slot_indices % MAXT_DEV < tile_count[owners]).astype(jnp.float32)
    stacked = jnp.concatenate([current_block, previous_block], axis=0)
    images = apply_operator(stacked, adjacency_tiles, tile_rows, tile_cols, live_mask)
    x_image = images[:K]
    p_image = images[K:]
    quotient = jnp.sum(current_block * x_image, axis=1) / (jnp.sum(current_block * current_block, axis=1) + 1e-06)
    frozen_rows = jnp.arange(K, dtype=jnp.int32) < locked[0]
    residual = jnp.where(frozen_rows[:, None], 0.0, x_image - quotient[:, None] * current_block)
    gram_w = inner_products(residual, residual) / NV + jnp.diag(frozen_rows.astype(jnp.float32))
    factor = jnp.linalg.cholesky(gram_w)
    w_basis = lax.linalg.triangular_solve(factor, residual, left_side=True, lower=True)
    w_image = apply_operator(w_basis, adjacency_tiles, tile_rows, tile_cols, live_mask)
    search = jnp.concatenate([current_block, w_basis, previous_block], axis=0)
    search_image = jnp.concatenate([x_image, w_image, p_image], axis=0)
    zero_rows = jnp.zeros((K,), jnp.float32)
    pad_diag = jnp.concatenate([zero_rows, frozen_rows.astype(jnp.float32), zero_rows])
    gram_b = inner_products(search, search) / NV + jnp.diag(pad_diag)
    gram_a = inner_products(search, search_image) / NV
    ritz_matrix = rayleigh_ritz(gram_b, gram_a)
    return (w_basis, w_image, ritz_matrix)
```

```python
import functools

import jax
import jax.numpy as jnp
from jax import lax
from jax.experimental import pallas as pl
from jax.experimental.pallas import tpu as pltpu
from jax.sharding import PartitionSpec as P

MESH = pl.DeviceIdType.MESH
F32 = jnp.float32
BF16 = jnp.bfloat16
HIGHEST = lax.Precision.HIGHEST
NT_DIMS = (((1,), (1,)), ((), ()))


def split(values):
    high = values.astype(BF16)
    return high, (values - high.astype(F32)).astype(BF16)


def iota(shape, dim):
    return lax.broadcasted_iota(jnp.int32, shape, dim)


def gather_kernel(
    sizes,
    cols_ref, rows_ref, count_ref, locked_ref, x_ref, p_ref, tiles_ref,
    r_ref, ar_ref, gram_ref,
    raw, halves, xh, ph, yh, q_buf, z_buf, extra, mine_q, near_q, line_q, far_q, mine_g, near_g, line_g, far_g,
    tile_sem, halo_send, halo_recv, near_send, near_recv, far_send, far_recv,
):
    row_count, col_count, sub_count = sizes
    near_count = col_count * sub_count
    vectors, here = x_ref.shape
    slots, tile, _ = tiles_ref.shape
    row_tiles = here // tile
    reach = row_tiles // 2
    spare = slots - row_tiles
    chunk = row_tiles // 2
    chunks = slots // chunk

    row_at = lax.axis_index("rows")
    near_at = lax.axis_index("cols") * sub_count + lax.axis_index("sub")
    position = row_at * near_count + near_at
    total = row_count * near_count

    def place(spot):
        return {
            "rows": spot // near_count,
            "cols": (spot % near_count) // sub_count,
            "sub": spot % sub_count,
        }

    def near_device(index):
        return {"cols": index // sub_count, "sub": index % sub_count}

    def far_device(index):
        return {"rows": index}

    tile_copies = []
    for c in range(chunks):
        part = pl.ds(c * chunk, chunk)
        tile_copies.append(pltpu.make_async_copy(tiles_ref.at[part], raw.at[part], tile_sem.at[c]))
        tile_copies[-1].start()

    has_left = position > 0
    has_right = position < total - 1
    barrier = pltpu.get_barrier_semaphore()

    @pl.when(has_left)
    def _():
        pl.semaphore_signal(barrier, inc=1, device_id=place(position - 1), device_id_type=MESH)

    @pl.when(has_right)
    def _():
        pl.semaphore_signal(barrier, inc=1, device_id=place(position + 1), device_id_type=MESH)

    for k in range(1, near_count):
        pl.semaphore_signal(
            barrier, inc=1, device_id=near_device((near_at + k) % near_count), device_id_type=MESH
        )
    for k in range(1, row_count):
        pl.semaphore_signal(
            barrier, inc=1, device_id=far_device((row_at + k) % row_count), device_id_type=MESH
        )
    for t in range(row_tiles):
        xh[reach + t] = x_ref[:, t * tile : (t + 1) * tile]
        ph[reach + t] = p_ref[:, t * tile : (t + 1) * tile]
    expected = near_count + row_count - 2
    pl.semaphore_wait(
        barrier, expected + has_left.astype(jnp.int32) + has_right.astype(jnp.int32)
    )

    def halo_copies(buffer, which):
        left = pltpu.make_async_remote_copy(
            src_ref=buffer.at[pl.ds(reach, reach)],
            dst_ref=buffer.at[pl.ds(reach + row_tiles, reach)],
            send_sem=halo_send.at[which, 0],
            recv_sem=halo_recv.at[which, 0],
            device_id=place(position - 1),
            device_id_type=MESH,
        )
        right = pltpu.make_async_remote_copy(
            src_ref=buffer.at[pl.ds(row_tiles, reach)],
            dst_ref=buffer.at[pl.ds(0, reach)],
            send_sem=halo_send.at[which, 1],
            recv_sem=halo_recv.at[which, 1],
            device_id=place(position + 1),
            device_id_type=MESH,
        )
        return left, right

    def halo_start(copies):
        left, right = copies

        @pl.when(has_left)
        def _():
            left.start()

        @pl.when(has_right)
        def _():
            right.start()

    def halo_arrived(copies):
        left, right = copies

        @pl.when(has_right)
        def _():
            left.wait_recv()

        @pl.when(has_left)
        def _():
            right.wait_recv()

    def halo_sent(copies):
        left, right = copies

        @pl.when(has_left)
        def _():
            left.wait_send()

        @pl.when(has_right)
        def _():
            right.wait_send()

    x_halo = halo_copies(xh, 0)
    p_halo = halo_copies(ph, 1)
    y_halo = halo_copies(yh, 2)
    halo_start(x_halo)
    halo_start(p_halo)

    def product(block, slot):
        high, low = split(block)
        lhs = jnp.concatenate(
            [jnp.concatenate([high, high], axis=1), jnp.concatenate([low, low], axis=1)], axis=0
        )
        out = jnp.dot(lhs, halves[slot], preferred_element_type=F32)
        return out[:vectors] + out[vectors:]

    def flat(buffer, start):
        return jnp.concatenate([buffer[start + t] for t in range(row_tiles)], axis=1)

    def split_tiles(c):
        tile_copies[c].wait()

        def step(i, carry):
            t = c * chunk + i
            high, low = split(raw[t])
            halves[t, 0:tile, :] = high
            halves[t, tile : 2 * tile, :] = low
            return carry

        lax.fori_loop(0, chunk, step, 0)

    def diagonal(source, target, target_base):
        def step(g, carry):
            for i in range(8):
                r = g * 8 + i
                target[target_base + r] = product(source[reach + r], r)
            return carry

        lax.fori_loop(0, row_tiles // 8, step, 0)

    live = count_ref[0]
    base_col = position * row_tiles - reach
    base_row = position * row_tiles
    places = [
        jnp.where(row_tiles + t < live, rows_ref[row_tiles + t] - base_row, -1) for t in range(spare)
    ]

    def scattered(padded, target, target_base):
        def step(g, carry):
            for i in range(8):
                t = g * 8 + i
                index = jnp.clip(cols_ref[row_tiles + t] - base_col, 0, 2 * row_tiles - 1)
                extra[t] = product(padded[index], row_tiles + t)
            return carry

        lax.fori_loop(0, spare // 8, step, 0)

        def gather(r, carry):
            sums = [target[target_base + r], None, None, None]
            for t in range(spare):
                term = extra[t] * jnp.where(places[t] == r, 1.0, 0.0).astype(F32)
                sums[t % 4] = term if sums[t % 4] is None else sums[t % 4] + term
            target[target_base + r] = (sums[0] + sums[1]) + (sums[2] + sums[3])
            return carry

        lax.fori_loop(0, row_tiles, gather, 0)

    def exchange(mine, buffer, count, at, device, send, recv, which):
        copies = []
        for k in range(1, count):
            other = (at + k) % count
            copies.append(
                (
                    pltpu.make_async_remote_copy(
                        src_ref=mine,
                        dst_ref=buffer.at[at],
                        send_sem=send.at[which, k],
                        recv_sem=recv.at[which, at],
                        device_id=device(other),
                        device_id_type=MESH,
                    ),
                    pltpu.make_async_remote_copy(
                        src_ref=mine,
                        dst_ref=buffer.at[other],
                        send_sem=send.at[which, k],
                        recv_sem=recv.at[which, other],
                        device_id=device(other),
                        device_id_type=MESH,
                    ),
                )
            )
        for out, _ in copies:
            out.start()
        buffer[at] = mine[...]
        return copies

    def collect(copies, buffer, count):
        for _, arriving in copies:
            arriving.wait_recv()
        out = buffer[0]
        for k in range(1, count):
            out = out + buffer[k]
        return out

    def flush(copies):
        for out, _ in copies:
            out.wait_send()

    for c in range(chunks):
        split_tiles(c)
        if c == row_tiles // chunk - 1:
            diagonal(xh, yh, reach)
    diagonal(ph, q_buf, 0)
    halo_arrived(x_halo)
    scattered(xh, yh, reach)
    halo_start(y_halo)

    x = x_ref[...]
    xx = jnp.sum(x * x, axis=1, keepdims=True)
    y = flat(yh, reach)
    xy = jnp.sum(x * y, axis=1, keepdims=True)
    lane = iota((vectors, 128), 1)
    line = iota((vectors, 128), 0)
    on_first = lane == line
    on_second = lane == line + vectors
    mine_q[...] = jnp.sum(
        jnp.where(on_first, xx, 0.0) + jnp.where(on_second, xy, 0.0), axis=0, keepdims=True
    )
    near_copies = exchange(mine_q, near_q, near_count, near_at, near_device, near_send, near_recv, 0)

    halo_arrived(p_halo)
    scattered(ph, q_buf, 0)

    line_q[...] = collect(near_copies, near_q, near_count)
    far_copies = exchange(line_q, far_q, row_count, row_at, far_device, far_send, far_recv, 0)
    diagonal(yh, z_buf, 0)
    halo_arrived(y_halo)
    scattered(yh, z_buf, 0)

    sums = jnp.broadcast_to(collect(far_copies, far_q, row_count), (vectors, 128))
    xx_all = jnp.sum(jnp.where(on_first, sums, 0.0), axis=1, keepdims=True)
    xy_all = jnp.sum(jnp.where(on_second, sums, 0.0), axis=1, keepdims=True)
    shift = (xy_all + 1e-06) / (xx_all + 1e-06)
    free = iota((vectors, 1), 0) >= locked_ref[0]
    y = flat(yh, reach)
    z = flat(z_buf, 0)
    p = p_ref[...]
    residual = jnp.where(free, shift * x - y, 0.0)
    residual_image = residual - jnp.where(free, shift * y - z, 0.0)
    r_ref[...] = residual
    ar_ref[...] = residual_image
    search = [split(v) for v in (x, residual, p)]
    image = [split(v) for v in (x - y, residual_image, p - flat(q_buf, 0))]
    left = jnp.concatenate([v[0] for v in search] + [v[1] for v in search], axis=0)
    right_high = jnp.concatenate([v[0] for v in search] + [v[0] for v in image], axis=0)
    right_low = jnp.concatenate([v[1] for v in search] + [v[1] for v in image], axis=0)
    full = lax.dot_general(left, right_high, NT_DIMS, preferred_element_type=F32)
    full = full + lax.dot_general(left, right_low, NT_DIMS, preferred_element_type=F32)
    width = 3 * vectors
    mine_g[...] = jnp.zeros_like(mine_g)
    mine_g[:, 0 : 2 * width] = full[:width] + full[width:]
    near_g_copies = exchange(
        mine_g, near_g, near_count, near_at, near_device, near_send, near_recv, 1
    )
    line_g[...] = collect(near_g_copies, near_g, near_count)
    far_g_copies = exchange(line_g, far_g, row_count, row_at, far_device, far_send, far_recv, 1)
    gram_ref[...] = collect(far_g_copies, far_g, row_count)

    halo_sent(x_halo)
    halo_sent(p_halo)
    halo_sent(y_halo)
    flush(near_copies)
    flush(far_copies)
    flush(near_g_copies)
    flush(far_g_copies)


def finish_kernel(vertex_total, locked_ref, r_ref, ar_ref, gram_ref, w_ref, aw_ref, ritz_ref, upper):
    vectors = r_ref.shape[0]
    width = 3 * vectors
    scale = 1.0 / vertex_total
    gram = gram_ref[...] * scale
    locked = locked_ref[0]

    lane = iota((width, 128), 1)
    line = iota((width, 128), 0)
    padded = (line == lane) & (line >= vectors) & (line < vectors + locked)
    big = jnp.where(lane < width, gram + jnp.where(padded, 1.0, 0.0), 0.0)
    big = big + jnp.where(lane == line + width, 1.0, 0.0)

    lane_w = iota((vectors, 128), 1)
    line_w = iota((vectors, 128), 0)
    frozen = (lane_w == line_w + vectors) & (line_w < locked)
    small = gram[vectors : 2 * vectors] + jnp.where(frozen, 1.0, 0.0)
    small = jnp.where((lane_w >= vectors) & (lane_w < 2 * vectors), small, 0.0)
    small = small + jnp.where(lane_w == line_w + 2 * vectors, 1.0, 0.0)

    def eliminate(matrix, k, pivot_lane):
        row = matrix[k : k + 1, :]
        pivot = row[:, pivot_lane : pivot_lane + 1]
        column = matrix[:, pivot_lane : pivot_lane + 1]
        return matrix - column * (row / pivot), row * lax.rsqrt(pivot)

    small_rows = []
    for k in range(vectors):
        small, row = eliminate(small, k, vectors + k)
        small_rows.append(row)
    inverse_w = jnp.concatenate(small_rows, axis=0)[:, 2 * vectors : 3 * vectors]
    w_ref[...] = jnp.dot(inverse_w, r_ref[...], precision=HIGHEST, preferred_element_type=F32)
    aw_ref[...] = jnp.dot(inverse_w, ar_ref[...], precision=HIGHEST, preferred_element_type=F32)

    for k in range(width):
        big, row = eliminate(big, k, k)
        upper[k : k + 1, :] = row
    inverse = upper[:, width : 2 * width]
    image = gram[:, width : 2 * width]
    half = jnp.dot(inverse, image, precision=HIGHEST, preferred_element_type=F32)
    first = lax.dot_general(half, inverse, NT_DIMS, precision=HIGHEST, preferred_element_type=F32)
    second = lax.dot_general(inverse, half, NT_DIMS, precision=HIGHEST, preferred_element_type=F32)
    ritz_ref[...] = 0.5 * (first + second)


def body(sizes, current_block, previous_block, adjacency_tiles, tile_rows, tile_cols, tile_count, locked):
    vectors, here = current_block.shape
    slots, tile, _ = adjacency_tiles.shape
    row_tiles = here // tile
    row_count, col_count, sub_count = sizes
    near_count = col_count * sub_count
    chunks = slots // (row_tiles // 2)
    width = 3 * vectors
    smem = pl.BlockSpec(memory_space=pltpu.SMEM)
    vmem = pl.BlockSpec(memory_space=pltpu.VMEM)
    anywhere = pl.BlockSpec(memory_space=pl.ANY)
    dma = pltpu.SemaphoreType.DMA
    residual, residual_image, gram = pl.pallas_call(
        functools.partial(gather_kernel, sizes),
        out_shape=(
            jax.ShapeDtypeStruct((vectors, here), F32),
            jax.ShapeDtypeStruct((vectors, here), F32),
            jax.ShapeDtypeStruct((width, 128), F32),
        ),
        in_specs=[smem] * 4 + [vmem] * 2 + [anywhere],
        out_specs=(vmem, vmem, vmem),
        scratch_shapes=[
            pltpu.VMEM((slots, tile, tile), F32),
            pltpu.VMEM((slots, 2 * tile, tile), BF16),
            pltpu.VMEM((2 * row_tiles, vectors, tile), F32),
            pltpu.VMEM((2 * row_tiles, vectors, tile), F32),
            pltpu.VMEM((2 * row_tiles, vectors, tile), F32),
            pltpu.VMEM((row_tiles, vectors, tile), F32),
            pltpu.VMEM((row_tiles, vectors, tile), F32),
            pltpu.VMEM((slots - row_tiles, vectors, tile), F32),
            pltpu.VMEM((1, 128), F32),
            pltpu.VMEM((near_count, 1, 128), F32),
            pltpu.VMEM((1, 128), F32),
            pltpu.VMEM((row_count, 1, 128), F32),
            pltpu.VMEM((width, 128), F32),
            pltpu.VMEM((near_count, width, 128), F32),
            pltpu.VMEM((width, 128), F32),
            pltpu.VMEM((row_count, width, 128), F32),
            dma((chunks,)),
            dma((3, 2)),
            dma((3, 2)),
            dma((2, near_count)),
            dma((2, near_count)),
            dma((2, row_count)),
            dma((2, row_count)),
        ],
        compiler_params=pltpu.CompilerParams(collective_id=0, has_side_effects=True),
        name="operator_and_grams",
    )(tile_cols, tile_rows, tile_count, locked, current_block, previous_block, adjacency_tiles)
    vertex_total = here * row_count * near_count
    return pl.pallas_call(
        functools.partial(finish_kernel, vertex_total),
        out_shape=(
            jax.ShapeDtypeStruct((vectors, here), F32),
            jax.ShapeDtypeStruct((vectors, here), F32),
            jax.ShapeDtypeStruct((width, width), F32),
        ),
        in_specs=[smem] + [vmem] * 3,
        out_specs=(vmem, vmem, vmem),
        scratch_shapes=[pltpu.VMEM((width, 128), F32)],
        name="factor_and_project",
    )(locked, residual, residual_image, gram)


def solution(mesh):
    split_all = ("graphs", "rows", "cols", "sub")
    sizes = tuple(mesh.shape[name] for name in ("rows", "cols", "sub"))
    in_specs = (
        P(None, split_all),
        P(None, split_all),
        P(split_all, None, None),
        P(split_all),
        P(split_all),
        P(split_all),
        P("graphs"),
    )
    out_specs = (P(None, split_all), P(None, split_all), P("graphs", None))
    return jax.shard_map(
        functools.partial(body, sizes), mesh=mesh, in_specs=in_specs, out_specs=out_specs, check_vma=False
    )
```

```python
import functools

import jax
import jax.numpy as jnp
from jax import lax
from jax.experimental import pallas as pl
from jax.experimental.pallas import tpu as pltpu
from jax.sharding import PartitionSpec as P

MESH = pl.DeviceIdType.MESH
F32 = jnp.float32
BF16 = jnp.bfloat16
HIGHEST = lax.Precision.HIGHEST
NT_DIMS = (((1,), (1,)), ((), ()))


def split(values):
    high = values.astype(BF16)
    return high, (values - high.astype(F32)).astype(BF16)


def iota(shape, dim):
    return lax.broadcasted_iota(jnp.int32, shape, dim)


def gather_kernel(
    sizes,
    cols_ref, rows_ref, count_ref, locked_ref, x_hbm, p_hbm, tiles_ref,
    r_ref, ar_ref, early_ref, late_ref,
    x_ref, p_ref, raw, halves, xh, ph, yh, q_buf, z_buf, extra, mine_q, near_q, line_q, far_q,
    mine_e, near_e, line_e, far_e, mine_g, near_g, line_g, far_g, block_sem, tile_sem, halo_send, halo_recv, near_send, near_recv, far_send, far_recv,
):
    row_count, col_count, sub_count = sizes
    near_count = col_count * sub_count
    vectors, here = x_ref.shape
    slots, tile, _ = tiles_ref.shape
    row_tiles = here // tile
    reach = row_tiles // 2
    spare = slots - row_tiles
    chunk = row_tiles // 2
    chunks = slots // chunk

    row_at = lax.axis_index("rows")
    near_at = lax.axis_index("cols") * sub_count + lax.axis_index("sub")
    position = row_at * near_count + near_at
    total = row_count * near_count

    def place(spot):
        return {
            "rows": spot // near_count,
            "cols": (spot % near_count) // sub_count,
            "sub": spot % sub_count,
        }

    def near_device(index):
        return {"cols": index // sub_count, "sub": index % sub_count}

    def far_device(index):
        return {"rows": index}

    block_copies = (
        pltpu.make_async_copy(x_hbm, x_ref, block_sem.at[0]),
        pltpu.make_async_copy(p_hbm, p_ref, block_sem.at[1]),
    )
    for copy in block_copies:
        copy.start()
    tile_copies = []
    for c in range(chunks):
        part = pl.ds(c * chunk, chunk)
        tile_copies.append(pltpu.make_async_copy(tiles_ref.at[part], raw.at[part], tile_sem.at[c]))
        tile_copies[-1].start()

    has_left = position > 0
    has_right = position < total - 1
    barrier = pltpu.get_barrier_semaphore()

    @pl.when(has_left)
    def _():
        pl.semaphore_signal(barrier, inc=1, device_id=place(position - 1), device_id_type=MESH)

    @pl.when(has_right)
    def _():
        pl.semaphore_signal(barrier, inc=1, device_id=place(position + 1), device_id_type=MESH)

    for k in range(1, near_count):
        pl.semaphore_signal(
            barrier, inc=1, device_id=near_device((near_at + k) % near_count), device_id_type=MESH
        )
    for k in range(1, row_count):
        pl.semaphore_signal(
            barrier, inc=1, device_id=far_device((row_at + k) % row_count), device_id_type=MESH
        )
    for copy in block_copies:
        copy.wait()
    for t in range(row_tiles):
        xh[reach + t] = x_ref[:, t * tile : (t + 1) * tile]
        ph[reach + t] = p_ref[:, t * tile : (t + 1) * tile]
    expected = near_count + row_count - 2
    pl.semaphore_wait(
        barrier, expected + has_left.astype(jnp.int32) + has_right.astype(jnp.int32)
    )

    def halo_copies(buffer, which):
        left = pltpu.make_async_remote_copy(
            src_ref=buffer.at[pl.ds(reach, reach)],
            dst_ref=buffer.at[pl.ds(reach + row_tiles, reach)],
            send_sem=halo_send.at[which, 0],
            recv_sem=halo_recv.at[which, 0],
            device_id=place(position - 1),
            device_id_type=MESH,
        )
        right = pltpu.make_async_remote_copy(
            src_ref=buffer.at[pl.ds(row_tiles, reach)],
            dst_ref=buffer.at[pl.ds(0, reach)],
            send_sem=halo_send.at[which, 1],
            recv_sem=halo_recv.at[which, 1],
            device_id=place(position + 1),
            device_id_type=MESH,
        )
        return left, right

    def halo_start(copies):
        left, right = copies

        @pl.when(has_left)
        def _():
            left.start()

        @pl.when(has_right)
        def _():
            right.start()

    def halo_arrived(copies):
        left, right = copies

        @pl.when(has_right)
        def _():
            left.wait_recv()

        @pl.when(has_left)
        def _():
            right.wait_recv()

    def halo_sent(copies):
        left, right = copies

        @pl.when(has_left)
        def _():
            left.wait_send()

        @pl.when(has_right)
        def _():
            right.wait_send()

    x_halo = halo_copies(xh, 0)
    p_halo = halo_copies(ph, 1)
    y_halo = halo_copies(yh, 2)
    halo_start(x_halo)
    halo_start(p_halo)

    def product(block, slot):
        high, low = split(block)
        lhs = jnp.concatenate(
            [jnp.concatenate([high, high], axis=1), jnp.concatenate([low, low], axis=1)], axis=0
        )
        out = jnp.dot(lhs, halves[slot], preferred_element_type=F32)
        return out[:vectors] + out[vectors:]

    def flat(buffer, start):
        return jnp.concatenate([buffer[start + t] for t in range(row_tiles)], axis=1)

    def split_tiles(c):
        tile_copies[c].wait()

        def step(i, carry):
            t = c * chunk + i
            high, low = split(raw[t])
            halves[t, 0:tile, :] = high
            halves[t, tile : 2 * tile, :] = low
            return carry

        lax.fori_loop(0, chunk, step, 0)

    def diagonal(source, target, target_base):
        def step(g, carry):
            for i in range(8):
                r = g * 8 + i
                target[target_base + r] = product(source[reach + r], r)
            return carry

        lax.fori_loop(0, row_tiles // 8, step, 0)

    live = count_ref[0]
    base_col = position * row_tiles - reach
    base_row = position * row_tiles
    places = [
        jnp.where(row_tiles + t < live, rows_ref[row_tiles + t] - base_row, -1) for t in range(spare)
    ]

    def scattered(padded, target, target_base):
        for t in range(spare):
            index = jnp.clip(cols_ref[row_tiles + t] - base_col, 0, 2 * row_tiles - 1)
            extra[t] = product(padded[index], row_tiles + t)

        def gather(g, carry):
            some = [g * 4 + i for i in range(4)]
            sums = [target[target_base + r] for r in some]
            for t in range(spare):
                block = extra[t]
                for i, r in enumerate(some):
                    sums[i] = sums[i] + block * jnp.where(places[t] == r, 1.0, 0.0).astype(F32)
            for i, r in enumerate(some):
                target[target_base + r] = sums[i]
            return carry

        lax.fori_loop(0, row_tiles // 4, gather, 0)

    def exchange(mine, buffer, count, at, device, send, recv, which):
        copies = []
        for k in range(1, count):
            other = (at + k) % count
            copies.append(
                (
                    pltpu.make_async_remote_copy(
                        src_ref=mine,
                        dst_ref=buffer.at[at],
                        send_sem=send.at[which, k],
                        recv_sem=recv.at[which, at],
                        device_id=device(other),
                        device_id_type=MESH,
                    ),
                    pltpu.make_async_remote_copy(
                        src_ref=mine,
                        dst_ref=buffer.at[other],
                        send_sem=send.at[which, k],
                        recv_sem=recv.at[which, other],
                        device_id=device(other),
                        device_id_type=MESH,
                    ),
                )
            )
        for out, _ in copies:
            out.start()
        buffer[at] = mine[...]
        return copies

    def collect(copies, buffer, count):
        for _, arriving in copies:
            arriving.wait_recv()
        out = buffer[0]
        for k in range(1, count):
            out = out + buffer[k]
        return out

    def flush(copies):
        for out, _ in copies:
            out.wait_send()

    for c in range(chunks):
        split_tiles(c)
        if c == row_tiles // chunk - 1:
            diagonal(xh, yh, reach)
    diagonal(ph, q_buf, 0)
    halo_arrived(x_halo)
    scattered(xh, yh, reach)
    halo_start(y_halo)

    x = x_ref[...]
    xx = jnp.sum(x * x, axis=1, keepdims=True)
    y = flat(yh, reach)
    xy = jnp.sum(x * y, axis=1, keepdims=True)
    lane = iota((vectors, 128), 1)
    line = iota((vectors, 128), 0)
    on_first = lane == line
    on_second = lane == line + vectors
    mine_q[...] = jnp.sum(
        jnp.where(on_first, xx, 0.0) + jnp.where(on_second, xy, 0.0), axis=0, keepdims=True
    )
    near_copies = exchange(mine_q, near_q, near_count, near_at, near_device, near_send, near_recv, 0)

    halo_arrived(p_halo)
    scattered(ph, q_buf, 0)
    p = p_ref[...]
    x_parts, y_parts, p_parts, q_parts = [split(v) for v in (x, y, p, flat(q_buf, 0))]
    gap = jnp.zeros((vectors, here), BF16)

    def inner(left, right):
        lhs = jnp.concatenate([v[0] for v in left] + [v[1] for v in left], axis=0)
        out = None
        for half in range(2):
            rhs = jnp.concatenate([gap if v is None else v[half] for v in right], axis=0)
            term = lax.dot_general(lhs, rhs, NT_DIMS, preferred_element_type=F32)
            out = term if out is None else out + term
        count = len(left) * vectors
        return out[:count] + out[count:]

    wide = 6 * vectors
    mine_e[...] = jnp.zeros_like(mine_e)
    mine_e[:, 0:wide] = inner(
        (x_parts, p_parts), (x_parts, None, p_parts, y_parts, None, q_parts)
    )
    near_e_copies = exchange(
        mine_e, near_e, near_count, near_at, near_device, near_send, near_recv, 1
    )

    line_q[...] = collect(near_copies, near_q, near_count)
    far_copies = exchange(line_q, far_q, row_count, row_at, far_device, far_send, far_recv, 0)
    diagonal(yh, z_buf, 0)
    line_e[...] = collect(near_e_copies, near_e, near_count)
    far_e_copies = exchange(line_e, far_e, row_count, row_at, far_device, far_send, far_recv, 1)
    halo_arrived(y_halo)
    scattered(yh, z_buf, 0)

    sums = jnp.broadcast_to(collect(far_copies, far_q, row_count), (vectors, 128))
    xx_all = jnp.sum(jnp.where(on_first, sums, 0.0), axis=1, keepdims=True)
    xy_all = jnp.sum(jnp.where(on_second, sums, 0.0), axis=1, keepdims=True)
    shift = (xy_all + 1e-06) / (xx_all + 1e-06)
    free = iota((vectors, 1), 0) >= locked_ref[0]
    residual = jnp.where(free, shift * x - y, 0.0)
    carried = jnp.where(free, shift * y - flat(z_buf, 0), 0.0)
    r_ref[...] = residual
    ar_ref[...] = residual - carried
    r_parts, n_parts = split(residual), split(carried)
    plain = inner((r_parts,), (x_parts, r_parts, p_parts, y_parts, n_parts, q_parts))
    other = inner((n_parts,), (x_parts, r_parts, p_parts, x_parts, r_parts, p_parts))
    first_half = iota((vectors, wide), 1) < 3 * vectors
    mine_g[...] = jnp.zeros_like(mine_g)
    mine_g[:, 0:wide] = jnp.where(first_half, plain, 0.5 * (plain + other))
    near_g_copies = exchange(
        mine_g, near_g, near_count, near_at, near_device, near_send, near_recv, 2
    )
    line_g[...] = collect(near_g_copies, near_g, near_count)
    far_g_copies = exchange(line_g, far_g, row_count, row_at, far_device, far_send, far_recv, 2)
    early_ref[...] = collect(far_e_copies, far_e, row_count)
    late_ref[...] = collect(far_g_copies, far_g, row_count)

    halo_sent(x_halo)
    halo_sent(p_halo)
    halo_sent(y_halo)
    flush(near_copies)
    flush(far_copies)
    flush(near_e_copies)
    flush(far_e_copies)
    flush(near_g_copies)
    flush(far_g_copies)


def finish_kernel(
    vertex_total, locked_ref, r_hbm, ar_hbm, early_ref, late_ref, w_hbm, aw_hbm, ritz_ref,
    upper, r_buf, ar_buf, w_buf, aw_buf, in_sem, out_sem,
):
    vectors = r_buf.shape[0]
    width = 3 * vectors
    ins = (
        pltpu.make_async_copy(r_hbm, r_buf, in_sem.at[0]),
        pltpu.make_async_copy(ar_hbm, ar_buf, in_sem.at[1]),
    )
    outs = (
        pltpu.make_async_copy(w_buf, w_hbm, out_sem.at[0]),
        pltpu.make_async_copy(aw_buf, aw_hbm, out_sem.at[1]),
    )
    for copy in ins:
        copy.start()
    scale = 1.0 / vertex_total
    early = early_ref[...] * scale
    late = late_ref[...] * scale
    locked = locked_ref[0]

    lane_w = iota((vectors, 128), 1)
    line_w = iota((vectors, 128), 0)
    frozen = (lane_w == line_w + vectors) & (line_w < locked)
    small = late + jnp.where(frozen, 1.0, 0.0)
    small = jnp.where((lane_w >= vectors) & (lane_w < 2 * vectors), small, 0.0)
    small = small + jnp.where(lane_w == line_w + 2 * vectors, 1.0, 0.0)

    lane = iota((width, 128), 1)
    line = iota((width, 128), 0)
    outer = (line < vectors) | (line >= 2 * vectors)
    pick = jnp.concatenate(
        [
            jnp.where(outer & (lane == line), 1.0, 0.0),
            jnp.where(outer & (lane == line + width), 1.0, 0.0),
        ],
        axis=1,
    )
    above = jnp.zeros((vectors, 128), F32)
    set_first = jnp.concatenate([above, late, above, above, above, above, above, above], axis=0)
    set_second = jnp.concatenate([above, above, above, above, late, above, above, above], axis=0)
    turned = lax.dot_general(
        pick, jnp.concatenate([set_first, set_second], axis=1), NT_DIMS,
        precision=HIGHEST, preferred_element_type=F32,
    )
    gram = jnp.concatenate([early[:vectors], late, early[vectors:]], axis=0) + turned
    padded = (line == lane) & (line >= vectors) & (line < vectors + locked)
    big = jnp.where(lane < width, gram + jnp.where(padded, 1.0, 0.0), 0.0)
    big = big + jnp.where(lane == line + width, 1.0, 0.0)

    def panel(matrix, k, shift, count):
        rows = [matrix[k + i : k + i + 1, :] for i in range(count)]
        columns = [
            jnp.broadcast_to(matrix[:, shift + k + i : shift + k + i + 1], matrix.shape)
            for i in range(count)
        ]
        block = {
            (i, j): jnp.broadcast_to(rows[i][:, shift + k + j : shift + k + j + 1], (1, 128))
            for i in range(count)
            for j in range(i, count)
        }
        done = []
        for m in range(count):
            inverse = 1.0 / block[m, m]
            done.append(rows[m] * lax.rsqrt(block[m, m]))
            factors = {j: block[m, j] * inverse for j in range(m + 1, count)}
            for i in range(m + 1, count):
                for j in range(i, count):
                    block[i, j] = block[i, j] - factors[i] * block[m, j]
                rows[i] = rows[i] - factors[i] * rows[m]
                columns[i] = columns[i] - factors[i] * columns[m]
            matrix = matrix - columns[m] * (rows[m] * inverse)
        return matrix, done

    step = 4
    small_rows = []
    for k in range(0, vectors, step):
        small, done = panel(small, k, vectors, step)
        small_rows += done
    inverse_w = jnp.concatenate(small_rows, axis=0)[:, 2 * vectors : 3 * vectors]
    for copy in ins:
        copy.wait()
    w_buf[...] = jnp.dot(inverse_w, r_buf[...], precision=HIGHEST, preferred_element_type=F32)
    outs[0].start()
    aw_buf[...] = jnp.dot(inverse_w, ar_buf[...], precision=HIGHEST, preferred_element_type=F32)
    outs[1].start()

    for k in range(0, width, step):
        big, done = panel(big, k, 0, step)
        for i in range(step):
            upper[k + i : k + i + 1, :] = done[i]
    inverse = upper[:, width : 2 * width]
    image = gram[:, :width] - gram[:, width : 2 * width]
    half = jnp.dot(inverse, image, precision=HIGHEST, preferred_element_type=F32)
    first = lax.dot_general(half, inverse, NT_DIMS, precision=HIGHEST, preferred_element_type=F32)
    second = lax.dot_general(inverse, half, NT_DIMS, precision=HIGHEST, preferred_element_type=F32)
    ritz_ref[...] = 0.5 * (first + second)
    for copy in outs:
        copy.wait()


def body(sizes, current_block, previous_block, adjacency_tiles, tile_rows, tile_cols, tile_count, locked):
    vectors, here = current_block.shape
    slots, tile, _ = adjacency_tiles.shape
    row_tiles = here // tile
    row_count, col_count, sub_count = sizes
    near_count = col_count * sub_count
    chunks = slots // (row_tiles // 2)
    width = 3 * vectors
    smem = pl.BlockSpec(memory_space=pltpu.SMEM)
    vmem = pl.BlockSpec(memory_space=pltpu.VMEM)
    anywhere = pl.BlockSpec(memory_space=pl.ANY)
    dma = pltpu.SemaphoreType.DMA
    residual, residual_image, early, late = pl.pallas_call(
        functools.partial(gather_kernel, sizes),
        out_shape=(
            jax.ShapeDtypeStruct((vectors, here), F32),
            jax.ShapeDtypeStruct((vectors, here), F32),
            jax.ShapeDtypeStruct((2 * vectors, 128), F32),
            jax.ShapeDtypeStruct((vectors, 128), F32),
        ),
        in_specs=[smem] * 4 + [anywhere] * 3,
        out_specs=(vmem, vmem, vmem, vmem),
        scratch_shapes=[
            pltpu.VMEM((vectors, here), F32),
            pltpu.VMEM((vectors, here), F32),
            pltpu.VMEM((slots, tile, tile), F32),
            pltpu.VMEM((slots, 2 * tile, tile), BF16),
            pltpu.VMEM((2 * row_tiles, vectors, tile), F32),
            pltpu.VMEM((2 * row_tiles, vectors, tile), F32),
            pltpu.VMEM((2 * row_tiles, vectors, tile), F32),
            pltpu.VMEM((row_tiles, vectors, tile), F32),
            pltpu.VMEM((row_tiles, vectors, tile), F32),
            pltpu.VMEM((slots - row_tiles, vectors, tile), F32),
            pltpu.VMEM((1, 128), F32),
            pltpu.VMEM((near_count, 1, 128), F32),
            pltpu.VMEM((1, 128), F32),
            pltpu.VMEM((row_count, 1, 128), F32),
            pltpu.VMEM((2 * vectors, 128), F32),
            pltpu.VMEM((near_count, 2 * vectors, 128), F32),
            pltpu.VMEM((2 * vectors, 128), F32),
            pltpu.VMEM((row_count, 2 * vectors, 128), F32),
            pltpu.VMEM((vectors, 128), F32),
            pltpu.VMEM((near_count, vectors, 128), F32),
            pltpu.VMEM((vectors, 128), F32),
            pltpu.VMEM((row_count, vectors, 128), F32),
            dma((2,)),
            dma((chunks,)),
            dma((3, 2)),
            dma((3, 2)),
            dma((3, near_count)),
            dma((3, near_count)),
            dma((3, row_count)),
            dma((3, row_count)),
        ],
        compiler_params=pltpu.CompilerParams(collective_id=0, has_side_effects=True),
        name="operator_and_grams",
    )(tile_cols, tile_rows, tile_count, locked, current_block, previous_block, adjacency_tiles)
    vertex_total = here * row_count * near_count
    return pl.pallas_call(
        functools.partial(finish_kernel, vertex_total),
        out_shape=(
            jax.ShapeDtypeStruct((vectors, here), F32),
            jax.ShapeDtypeStruct((vectors, here), F32),
            jax.ShapeDtypeStruct((width, width), F32),
        ),
        in_specs=[smem] + [anywhere] * 2 + [vmem] * 2,
        out_specs=(anywhere, anywhere, vmem),
        scratch_shapes=[pltpu.VMEM((width, 128), F32)]
        + [pltpu.VMEM((vectors, here), F32)] * 4
        + [dma((2,)), dma((2,))],
        name="factor_and_project",
    )(locked, residual, residual_image, early, late)


def solution(mesh):
    split_all = ("graphs", "rows", "cols", "sub")
    sizes = tuple(mesh.shape[name] for name in ("rows", "cols", "sub"))
    in_specs = (
        P(None, split_all),
        P(None, split_all),
        P(split_all, None, None),
        P(split_all),
        P(split_all),
        P(split_all),
        P("graphs"),
    )
    out_specs = (P(None, split_all), P(None, split_all), P("graphs", None))
    return jax.shard_map(
        functools.partial(body, sizes), mesh=mesh, in_specs=in_specs, out_specs=out_specs, check_vma=False
    )
```

```python
import functools

import jax
import jax.numpy as jnp
from jax import lax
from jax.experimental import pallas as pl
from jax.experimental.pallas import tpu as pltpu
from jax.sharding import PartitionSpec as P

MESH = pl.DeviceIdType.MESH
F32 = jnp.float32
BF16 = jnp.bfloat16
HIGHEST = lax.Precision.HIGHEST
NT_DIMS = (((1,), (1,)), ((), ()))


def split(values):
    high = values.astype(BF16)
    return high, (values - high.astype(F32)).astype(BF16)


def iota(shape, dim):
    return lax.broadcasted_iota(jnp.int32, shape, dim)


def gather_kernel(
    sizes,
    cols_ref, rows_ref, count_ref, locked_ref, x_hbm, p_hbm, tiles_ref,
    r_hbm, ar_hbm, early_ref, late_ref,
    x_ref, p_ref, r_ref, ar_ref, raw, halves, xh, ph, yh, q_buf, z_buf, extra, mine_q, near_q, line_q, far_q,
    mine_e, near_e, line_e, far_e, mine_g, near_g, line_g, far_g, block_sem, out_sem, tile_sem, halo_send, halo_recv, near_send, near_recv, far_send, far_recv,
):
    row_count, col_count, sub_count = sizes
    near_count = col_count * sub_count
    vectors, here = x_ref.shape
    slots, tile, _ = tiles_ref.shape
    row_tiles = here // tile
    reach = row_tiles // 2
    spare = slots - row_tiles
    chunk = row_tiles // 2
    chunks = slots // chunk

    row_at = lax.axis_index("rows")
    near_at = lax.axis_index("cols") * sub_count + lax.axis_index("sub")
    position = row_at * near_count + near_at
    total = row_count * near_count

    def place(spot):
        return {
            "rows": spot // near_count,
            "cols": (spot % near_count) // sub_count,
            "sub": spot % sub_count,
        }

    def near_device(index):
        return {"cols": index // sub_count, "sub": index % sub_count}

    def far_device(index):
        return {"rows": index}

    block_copies = (
        pltpu.make_async_copy(x_hbm, x_ref, block_sem.at[0]),
        pltpu.make_async_copy(p_hbm, p_ref, block_sem.at[1]),
    )
    for copy in block_copies:
        copy.start()
    tile_copies = []
    for c in range(chunks):
        part = pl.ds(c * chunk, chunk)
        tile_copies.append(pltpu.make_async_copy(tiles_ref.at[part], raw.at[part], tile_sem.at[c]))
        tile_copies[-1].start()

    has_left = position > 0
    has_right = position < total - 1
    barrier = pltpu.get_barrier_semaphore()

    @pl.when(has_left)
    def _():
        pl.semaphore_signal(barrier, inc=1, device_id=place(position - 1), device_id_type=MESH)

    @pl.when(has_right)
    def _():
        pl.semaphore_signal(barrier, inc=1, device_id=place(position + 1), device_id_type=MESH)

    for k in range(1, near_count):
        pl.semaphore_signal(
            barrier, inc=1, device_id=near_device((near_at + k) % near_count), device_id_type=MESH
        )
    for k in range(1, row_count):
        pl.semaphore_signal(
            barrier, inc=1, device_id=far_device((row_at + k) % row_count), device_id_type=MESH
        )
    for copy in block_copies:
        copy.wait()
    for t in range(row_tiles):
        xh[reach + t] = x_ref[:, t * tile : (t + 1) * tile]
        ph[reach + t] = p_ref[:, t * tile : (t + 1) * tile]
    expected = near_count + row_count - 2
    pl.semaphore_wait(
        barrier, expected + has_left.astype(jnp.int32) + has_right.astype(jnp.int32)
    )

    def halo_copies(buffer, which):
        left = pltpu.make_async_remote_copy(
            src_ref=buffer.at[pl.ds(reach, reach)],
            dst_ref=buffer.at[pl.ds(reach + row_tiles, reach)],
            send_sem=halo_send.at[which, 0],
            recv_sem=halo_recv.at[which, 0],
            device_id=place(position - 1),
            device_id_type=MESH,
        )
        right = pltpu.make_async_remote_copy(
            src_ref=buffer.at[pl.ds(row_tiles, reach)],
            dst_ref=buffer.at[pl.ds(0, reach)],
            send_sem=halo_send.at[which, 1],
            recv_sem=halo_recv.at[which, 1],
            device_id=place(position + 1),
            device_id_type=MESH,
        )
        return left, right

    def halo_start(copies):
        left, right = copies

        @pl.when(has_left)
        def _():
            left.start()

        @pl.when(has_right)
        def _():
            right.start()

    def halo_arrived(copies):
        left, right = copies

        @pl.when(has_right)
        def _():
            left.wait_recv()

        @pl.when(has_left)
        def _():
            right.wait_recv()

    def halo_sent(copies):
        left, right = copies

        @pl.when(has_left)
        def _():
            left.wait_send()

        @pl.when(has_right)
        def _():
            right.wait_send()

    x_halo = halo_copies(xh, 0)
    p_halo = halo_copies(ph, 1)
    y_halo = halo_copies(yh, 2)
    halo_start(x_halo)
    halo_start(p_halo)

    def product(block, slot):
        high, low = split(block)
        lhs = jnp.concatenate(
            [jnp.concatenate([high, high], axis=1), jnp.concatenate([low, low], axis=1)], axis=0
        )
        out = jnp.dot(lhs, halves[slot], preferred_element_type=F32)
        return out[:vectors] + out[vectors:]

    def flat(buffer, start):
        return jnp.concatenate([buffer[start + t] for t in range(row_tiles)], axis=1)

    def split_tiles(c):
        tile_copies[c].wait()

        def step(i, carry):
            t = c * chunk + i
            high, low = split(raw[t])
            halves[t, 0:tile, :] = high
            halves[t, tile : 2 * tile, :] = low
            return carry

        lax.fori_loop(0, chunk, step, 0)

    def diagonal(source, target, target_base):
        def step(g, carry):
            for i in range(8):
                r = g * 8 + i
                target[target_base + r] = product(source[reach + r], r)
            return carry

        lax.fori_loop(0, row_tiles // 8, step, 0)

    live = count_ref[0]
    base_col = position * row_tiles - reach
    base_row = position * row_tiles
    places = [
        jnp.where(row_tiles + t < live, rows_ref[row_tiles + t] - base_row, -1) for t in range(spare)
    ]

    def scattered(padded, target, target_base):
        for t in range(spare):
            index = jnp.clip(cols_ref[row_tiles + t] - base_col, 0, 2 * row_tiles - 1)
            extra[t] = product(padded[index], row_tiles + t)

        def gather(g, carry):
            some = [g * 4 + i for i in range(4)]
            sums = [target[target_base + r] for r in some]
            for t in range(spare):
                block = extra[t]
                for i, r in enumerate(some):
                    sums[i] = sums[i] + block * jnp.where(places[t] == r, 1.0, 0.0).astype(F32)
            for i, r in enumerate(some):
                target[target_base + r] = sums[i]
            return carry

        lax.fori_loop(0, row_tiles // 4, gather, 0)

    def exchange(mine, buffer, count, at, device, send, recv, which):
        copies = []
        for k in range(1, count):
            other = (at + k) % count
            copies.append(
                (
                    pltpu.make_async_remote_copy(
                        src_ref=mine,
                        dst_ref=buffer.at[at],
                        send_sem=send.at[which, k],
                        recv_sem=recv.at[which, at],
                        device_id=device(other),
                        device_id_type=MESH,
                    ),
                    pltpu.make_async_remote_copy(
                        src_ref=mine,
                        dst_ref=buffer.at[other],
                        send_sem=send.at[which, k],
                        recv_sem=recv.at[which, other],
                        device_id=device(other),
                        device_id_type=MESH,
                    ),
                )
            )
        for out, _ in copies:
            out.start()
        buffer[at] = mine[...]
        return copies

    def collect(copies, buffer, count):
        for _, arriving in copies:
            arriving.wait_recv()
        out = buffer[0]
        for k in range(1, count):
            out = out + buffer[k]
        return out

    def flush(copies):
        for out, _ in copies:
            out.wait_send()

    for c in range(chunks):
        split_tiles(c)
        if c == row_tiles // chunk - 1:
            diagonal(xh, yh, reach)
    diagonal(ph, q_buf, 0)
    halo_arrived(x_halo)
    scattered(xh, yh, reach)
    halo_start(y_halo)

    x = x_ref[...]
    xx = jnp.sum(x * x, axis=1, keepdims=True)
    y = flat(yh, reach)
    xy = jnp.sum(x * y, axis=1, keepdims=True)
    lane = iota((vectors, 128), 1)
    line = iota((vectors, 128), 0)
    on_first = lane == line
    on_second = lane == line + vectors
    mine_q[...] = jnp.sum(
        jnp.where(on_first, xx, 0.0) + jnp.where(on_second, xy, 0.0), axis=0, keepdims=True
    )
    near_copies = exchange(mine_q, near_q, near_count, near_at, near_device, near_send, near_recv, 0)

    halo_arrived(p_halo)
    scattered(ph, q_buf, 0)
    p = p_ref[...]
    x_parts, y_parts, p_parts, q_parts = [split(v) for v in (x, y, p, flat(q_buf, 0))]
    gap = jnp.zeros((vectors, here), BF16)

    def inner(left, right):
        lhs = jnp.concatenate([v[0] for v in left] + [v[1] for v in left], axis=0)
        out = None
        for half in range(2):
            rhs = jnp.concatenate([gap if v is None else v[half] for v in right], axis=0)
            term = lax.dot_general(lhs, rhs, NT_DIMS, preferred_element_type=F32)
            out = term if out is None else out + term
        count = len(left) * vectors
        return out[:count] + out[count:]

    wide = 6 * vectors
    mine_e[...] = jnp.zeros_like(mine_e)
    mine_e[:, 0:wide] = inner(
        (x_parts, p_parts), (x_parts, None, p_parts, y_parts, None, q_parts)
    )
    near_e_copies = exchange(
        mine_e, near_e, near_count, near_at, near_device, near_send, near_recv, 1
    )

    line_q[...] = collect(near_copies, near_q, near_count)
    far_copies = exchange(line_q, far_q, row_count, row_at, far_device, far_send, far_recv, 0)
    diagonal(yh, z_buf, 0)
    halo_arrived(y_halo)
    scattered(yh, z_buf, 0)

    sums = jnp.broadcast_to(collect(far_copies, far_q, row_count), (vectors, 128))
    xx_all = jnp.sum(jnp.where(on_first, sums, 0.0), axis=1, keepdims=True)
    xy_all = jnp.sum(jnp.where(on_second, sums, 0.0), axis=1, keepdims=True)
    shift = (xy_all + 1e-06) / (xx_all + 1e-06)
    free = iota((vectors, 1), 0) >= locked_ref[0]
    residual = jnp.where(free, shift * x - y, 0.0)
    carried = jnp.where(free, shift * y - flat(z_buf, 0), 0.0)
    r_ref[...] = residual
    ar_ref[...] = residual - carried
    outs = (
        pltpu.make_async_copy(r_ref, r_hbm, out_sem.at[0]),
        pltpu.make_async_copy(ar_ref, ar_hbm, out_sem.at[1]),
    )
    for copy in outs:
        copy.start()
    r_parts, n_parts = split(residual), split(carried)
    plain = inner((r_parts,), (x_parts, r_parts, p_parts, y_parts, n_parts, q_parts))
    other = inner((n_parts,), (x_parts, r_parts, p_parts, x_parts, r_parts, p_parts))
    first_half = iota((vectors, wide), 1) < 3 * vectors
    mine_g[...] = jnp.zeros_like(mine_g)
    mine_g[:, 0:wide] = jnp.where(first_half, plain, 0.5 * (plain + other))
    near_g_copies = exchange(
        mine_g, near_g, near_count, near_at, near_device, near_send, near_recv, 2
    )
    line_e[...] = collect(near_e_copies, near_e, near_count)
    far_e_copies = exchange(line_e, far_e, row_count, row_at, far_device, far_send, far_recv, 1)
    line_g[...] = collect(near_g_copies, near_g, near_count)
    far_g_copies = exchange(line_g, far_g, row_count, row_at, far_device, far_send, far_recv, 2)
    early_ref[...] = collect(far_e_copies, far_e, row_count)
    late_ref[...] = collect(far_g_copies, far_g, row_count)

    for copy in outs:
        copy.wait()
    halo_sent(x_halo)
    halo_sent(p_halo)
    halo_sent(y_halo)
    flush(near_copies)
    flush(far_copies)
    flush(near_e_copies)
    flush(far_e_copies)
    flush(near_g_copies)
    flush(far_g_copies)


def finish_kernel(
    vertex_total, locked_ref, r_hbm, ar_hbm, early_ref, late_ref, w_hbm, aw_hbm, ritz_ref,
    upper, r_buf, ar_buf, w_buf, aw_buf, in_sem, out_sem,
):
    vectors = r_buf.shape[0]
    width = 3 * vectors
    ins = (
        pltpu.make_async_copy(r_hbm, r_buf, in_sem.at[0]),
        pltpu.make_async_copy(ar_hbm, ar_buf, in_sem.at[1]),
    )
    outs = (
        pltpu.make_async_copy(w_buf, w_hbm, out_sem.at[0]),
        pltpu.make_async_copy(aw_buf, aw_hbm, out_sem.at[1]),
    )
    for copy in ins:
        copy.start()
    scale = 1.0 / vertex_total
    early = early_ref[...] * scale
    late = late_ref[...] * scale
    locked = locked_ref[0]

    lane_w = iota((vectors, 128), 1)
    line_w = iota((vectors, 128), 0)
    frozen = (lane_w == line_w + vectors) & (line_w < locked)
    small = late + jnp.where(frozen, 1.0, 0.0)
    small = jnp.where((lane_w >= vectors) & (lane_w < 2 * vectors), small, 0.0)
    small = small + jnp.where(lane_w == line_w + 2 * vectors, 1.0, 0.0)

    lane = iota((width, 128), 1)
    line = iota((width, 128), 0)
    outer = (line < vectors) | (line >= 2 * vectors)
    pick = jnp.concatenate(
        [
            jnp.where(outer & (lane == line), 1.0, 0.0),
            jnp.where(outer & (lane == line + width), 1.0, 0.0),
        ],
        axis=1,
    )
    above = jnp.zeros((vectors, 128), F32)
    set_first = jnp.concatenate([above, late, above, above, above, above, above, above], axis=0)
    set_second = jnp.concatenate([above, above, above, above, late, above, above, above], axis=0)
    turned = lax.dot_general(
        pick, jnp.concatenate([set_first, set_second], axis=1), NT_DIMS,
        precision=HIGHEST, preferred_element_type=F32,
    )
    gram = jnp.concatenate([early[:vectors], late, early[vectors:]], axis=0) + turned
    padded = (line == lane) & (line >= vectors) & (line < vectors + locked)
    big = jnp.where(lane < width, gram + jnp.where(padded, 1.0, 0.0), 0.0)
    big = big + jnp.where(lane == line + width, 1.0, 0.0)

    def panel(matrix, k, shift, count):
        rows = [matrix[k + i : k + i + 1, :] for i in range(count)]
        columns = [
            jnp.broadcast_to(matrix[:, shift + k + i : shift + k + i + 1], matrix.shape)
            for i in range(count)
        ]
        block = {
            (i, j): jnp.broadcast_to(rows[i][:, shift + k + j : shift + k + j + 1], (1, 128))
            for i in range(count)
            for j in range(i, count)
        }
        done = []
        for m in range(count):
            inverse = 1.0 / block[m, m]
            done.append(rows[m] * lax.rsqrt(block[m, m]))
            factors = {j: block[m, j] * inverse for j in range(m + 1, count)}
            for i in range(m + 1, count):
                for j in range(i, count):
                    block[i, j] = block[i, j] - factors[i] * block[m, j]
                rows[i] = rows[i] - factors[i] * rows[m]
                columns[i] = columns[i] - factors[i] * columns[m]
            matrix = matrix - columns[m] * (rows[m] * inverse)
        return matrix, done

    for copy in ins:
        copy.wait()
    step = 4
    small_rows = []
    for k in range(0, vectors, step):
        small, done = panel(small, k, vectors, step)
        small_rows += done
    inverse_w = jnp.concatenate(small_rows, axis=0)[:, 2 * vectors : 3 * vectors]
    for k in range(0, width, step):
        if k == 2 * vectors:
            w_buf[...] = jnp.dot(
                inverse_w, r_buf[...], precision=HIGHEST, preferred_element_type=F32
            )
            aw_buf[...] = jnp.dot(
                inverse_w, ar_buf[...], precision=HIGHEST, preferred_element_type=F32
            )
            for copy in outs:
                copy.start()
        big, done = panel(big, k, 0, step)
        for i in range(step):
            upper[k + i : k + i + 1, :] = done[i]
    inverse = upper[:, width : 2 * width]
    image = gram[:, :width] - gram[:, width : 2 * width]
    half = jnp.dot(inverse, image, precision=HIGHEST, preferred_element_type=F32)
    first = lax.dot_general(half, inverse, NT_DIMS, precision=HIGHEST, preferred_element_type=F32)
    second = lax.dot_general(inverse, half, NT_DIMS, precision=HIGHEST, preferred_element_type=F32)
    ritz_ref[...] = 0.5 * (first + second)
    for copy in outs:
        copy.wait()


def body(sizes, current_block, previous_block, adjacency_tiles, tile_rows, tile_cols, tile_count, locked):
    vectors, here = current_block.shape
    slots, tile, _ = adjacency_tiles.shape
    row_tiles = here // tile
    row_count, col_count, sub_count = sizes
    near_count = col_count * sub_count
    chunks = slots // (row_tiles // 2)
    width = 3 * vectors
    smem = pl.BlockSpec(memory_space=pltpu.SMEM)
    vmem = pl.BlockSpec(memory_space=pltpu.VMEM)
    anywhere = pl.BlockSpec(memory_space=pl.ANY)
    dma = pltpu.SemaphoreType.DMA
    residual, residual_image, early, late = pl.pallas_call(
        functools.partial(gather_kernel, sizes),
        out_shape=(
            jax.ShapeDtypeStruct((vectors, here), F32),
            jax.ShapeDtypeStruct((vectors, here), F32),
            jax.ShapeDtypeStruct((2 * vectors, 128), F32),
            jax.ShapeDtypeStruct((vectors, 128), F32),
        ),
        in_specs=[smem] * 4 + [anywhere] * 3,
        out_specs=(anywhere, anywhere, vmem, vmem),
        scratch_shapes=[
            pltpu.VMEM((vectors, here), F32),
            pltpu.VMEM((vectors, here), F32),
            pltpu.VMEM((vectors, here), F32),
            pltpu.VMEM((vectors, here), F32),
            pltpu.VMEM((slots, tile, tile), F32),
            pltpu.VMEM((slots, 2 * tile, tile), BF16),
            pltpu.VMEM((2 * row_tiles, vectors, tile), F32),
            pltpu.VMEM((2 * row_tiles, vectors, tile), F32),
            pltpu.VMEM((2 * row_tiles, vectors, tile), F32),
            pltpu.VMEM((row_tiles, vectors, tile), F32),
            pltpu.VMEM((row_tiles, vectors, tile), F32),
            pltpu.VMEM((slots - row_tiles, vectors, tile), F32),
            pltpu.VMEM((1, 128), F32),
            pltpu.VMEM((near_count, 1, 128), F32),
            pltpu.VMEM((1, 128), F32),
            pltpu.VMEM((row_count, 1, 128), F32),
            pltpu.VMEM((2 * vectors, 128), F32),
            pltpu.VMEM((near_count, 2 * vectors, 128), F32),
            pltpu.VMEM((2 * vectors, 128), F32),
            pltpu.VMEM((row_count, 2 * vectors, 128), F32),
            pltpu.VMEM((vectors, 128), F32),
            pltpu.VMEM((near_count, vectors, 128), F32),
            pltpu.VMEM((vectors, 128), F32),
            pltpu.VMEM((row_count, vectors, 128), F32),
            dma((2,)),
            dma((2,)),
            dma((chunks,)),
            dma((3, 2)),
            dma((3, 2)),
            dma((3, near_count)),
            dma((3, near_count)),
            dma((3, row_count)),
            dma((3, row_count)),
        ],
        compiler_params=pltpu.CompilerParams(collective_id=0, has_side_effects=True),
        name="operator_and_grams",
    )(tile_cols, tile_rows, tile_count, locked, current_block, previous_block, adjacency_tiles)
    vertex_total = here * row_count * near_count
    return pl.pallas_call(
        functools.partial(finish_kernel, vertex_total),
        out_shape=(
            jax.ShapeDtypeStruct((vectors, here), F32),
            jax.ShapeDtypeStruct((vectors, here), F32),
            jax.ShapeDtypeStruct((width, width), F32),
        ),
        in_specs=[smem] + [anywhere] * 2 + [vmem] * 2,
        out_specs=(anywhere, anywhere, vmem),
        scratch_shapes=[pltpu.VMEM((width, 128), F32)]
        + [pltpu.VMEM((vectors, here), F32)] * 4
        + [dma((2,)), dma((2,))],
        name="factor_and_project",
    )(locked, residual, residual_image, early, late)


def solution(mesh):
    split_all = ("graphs", "rows", "cols", "sub")
    sizes = tuple(mesh.shape[name] for name in ("rows", "cols", "sub"))
    in_specs = (
        P(None, split_all),
        P(None, split_all),
        P(split_all, None, None),
        P(split_all),
        P(split_all),
        P(split_all),
        P("graphs"),
    )
    out_specs = (P(None, split_all), P(None, split_all), P("graphs", None))
    return jax.shard_map(
        functools.partial(body, sizes), mesh=mesh, in_specs=in_specs, out_specs=out_specs, check_vma=False
    )
```
